32 devices in a mesh: dp: 8 (over z, x), layer: 4 (over y, core).
Axes of the slice: x: 2, y: 2, z: 4, core: 2. Of those that a mesh axis runs over, the one named last changes fastest.
Arguments:
- acts: bfloat16 [4, 7168, 4608], P('layer', 'dp')
- probes: bfloat16 [4, 4608, 512], P('layer'), may hold values from -0.25 to 0.25
- labels: int32 [7168], P('dp'), may hold values from 0 to 511
Outputs:
- grads: float32 [4, 4608, 512], P('layer', 'dp')
- losses: float32 [4], P('layer')
The draws below stay inside these ranges and needn't reach their ends.
All inputs are finite; a program needn't handle non-finite values.
Results may differ from the reference program's by a relative error of at most 0.0013.
Values sent between devices are 32-bit elements; how exact they have to be, the bound alone decides.
No kernel may reach another device: no remote copies, remote signals or barrier semaphores. Data moves between devices by JAX's collectives and lax.ppermute only.
A program may use at most 128 MiB of HBM per device.

```python
import jax
import jax.numpy as jnp
from jax import lax

D = 4608
C = 512
TOKENS = 7168
LAYERS = 4


def draw_acts(key, part):
    first = jax.random.fold_in(key, 0)
    base = jax.random.normal(first, (LAYERS, TOKENS, D), jnp.float32)
    base = jnp.clip(base, -6.0, 6.0)
    return base.astype(jnp.bfloat16)


def plant(entries, stream_key, low, high):
    extent = entries.shape
    spot = [jax.random.randint(jax.random.fold_in(stream_key, axis), (), 0, extent[axis]) for axis in range(len(extent))]
    entries = entries.at[tuple(spot)].set(low)
    longest = extent.index(max(extent))
    spot[longest] = (spot[longest] + 1) % extent[longest]
    return entries.at[tuple(spot)].set(high)


def levels(rng, shape, cuts, low, largest):
    level, own = 1.0, jax.random.fold_in(rng, 6)
    for dim, shards_of in cuts:
        steps = jnp.exp(jax.random.uniform(jax.random.fold_in(own, dim), (shards_of,), jnp.float32, low / len(cuts), largest / len(cuts)))
        level = level * jnp.repeat(steps, shape[dim] // shards_of).reshape([-1 if axis == dim else 1 for axis in range(len(shape))])
    return level


def noise(own_key, dims, scale, most, cuts=(), held_as=jnp.bfloat16):
    level = levels(own_key, dims, cuts, -0.22, 0.18) if cuts else 1.0
    array = jax.random.normal(own_key, dims, jnp.float32) * scale * level
    return jnp.minimum(jnp.maximum(array, -most), most).astype(held_as)


def setup_inputs(seed: int = 0) -> dict:
    seeds = jax.random.split(jax.random.key(seed), 4)
    return {
        "acts": draw_acts(jax.random.fold_in(seeds[3], 71), 0),
        "probes": noise(seeds[1], (LAYERS, D, C), (D // 9) ** -0.5, 0.25, ((0, 4),)),
        "labels": plant(jax.random.randint(seeds[2], (TOKENS,), 0, C), jax.random.fold_in(seeds[2], 1), 0, C - 1).astype(jnp.int32),
    }


def one_layer(item):
    acts_l, probe_l, onehot = item
    logits = jnp.dot(acts_l, probe_l, preferred_element_type=jnp.float32)
    top = jnp.max(logits, axis=1, keepdims=True)
    expo = jnp.exp(logits - top)
    total = jnp.sum(expo, axis=1, keepdims=True)
    probs = expo / total
    lse = top[:, 0] + jnp.log(total[:, 0])
    picked = jnp.sum(onehot * logits, axis=1)
    loss = jnp.sum(lse - picked) / jnp.float32(TOKENS)
    resid = (probs - onehot).astype(jnp.bfloat16)
    grad = lax.dot_general(acts_l, resid, (((0,), (0,)), ((), ())), preferred_element_type=jnp.float32)
    grad = grad * jnp.float32(1.0 / (TOKENS ** 0.5))
    return grad, loss


def reference(acts, probes, labels):
    classes = jnp.arange(C, dtype=jnp.int32)
    onehot = (labels[:, None] == classes[None, :]).astype(jnp.float32)

    def step(item):
        return one_layer((item[0], item[1], onehot))

    grads, losses = lax.map(step, (acts, probes))
    return grads, losses
```

```python
import functools

import jax
import jax.numpy as jnp
from jax import lax
from jax.experimental import pallas as pl
from jax.experimental.pallas import tpu as pltpu
from jax.sharding import PartitionSpec as P


LANES = 128
SUB = 8
LINE = 4
STEP = 512
ANY = pl.BlockSpec(memory_space=pl.ANY)
TN = (((0,), (0,)), ((), ()))


def layer_terms(acts_l, probe_l, onehot):
    logits = jnp.dot(acts_l, probe_l, preferred_element_type=jnp.float32)
    top = jnp.max(logits, axis=1, keepdims=True)
    expo = jnp.exp(logits - top)
    total = jnp.sum(expo, axis=1, keepdims=True)
    probs = expo / total
    lse = top[:, 0] + jnp.log(total[:, 0])
    picked = jnp.sum(onehot * logits, axis=1)
    resid = (probs - onehot).astype(jnp.bfloat16)
    return (resid, jnp.sum(lse - picked))


def plain(acts, probes, labels):
    count_all = acts.shape[1] * lax.axis_size("dp")
    factor = jnp.float32(1.0 / count_all**0.5)
    classes = jnp.arange(probes.shape[2], dtype=jnp.int32)
    onehot = (labels[:, None] == classes[None, :]).astype(jnp.float32)
    resid, loss = layer_terms(acts[0], probes[0], onehot)
    part = lax.dot_general(acts[0], resid, TN, preferred_element_type=jnp.float32) * factor
    grads = lax.psum_scatter(part, "dp", scatter_dimension=0, tiled=True)
    losses = lax.psum(loss[None], "dp") / jnp.float32(count_all)
    return (grads[None], losses)


def place():
    i = lax.axis_index("dp")
    z, x = i // 2, i % 2
    near = z < 2
    outer = jnp.logical_or(z == 0, z == LINE - 1)
    own = jnp.where(outer, 0, 1)

    def at(dist):
        return jnp.where(near, dist, LINE - 1 - dist)

    return x, at(3), at(2), at(1 - own), at(own)


def first_kernel(factor, acts, probes, labels, resid_o, x0_o, e_o, loss_o, acts_v, probes_v, labels_v, acc, resid_v, prod, loss_v, sem_a, sem_p, sem_l, sem_o):
    tok, wide = acts.shape
    classes = probes.shape[1]
    steps = wide // STEP
    half = e_o.shape[0]
    rows = 2 * half

    def acts_copy(k):
        cols = pl.ds(pl.multiple_of(k * STEP, STEP), STEP)
        return pltpu.make_async_copy(acts.at[:, cols], acts_v.at[:, cols], sem_a.at[k])

    def probes_copy(k):
        cols = pl.ds(pl.multiple_of(k * STEP, STEP), STEP)
        return pltpu.make_async_copy(probes.at[cols], probes_v.at[cols], sem_p.at[k])

    groups = tok // LANES
    label_copy = pltpu.make_async_copy(labels, labels_v.at[pl.ds(0, groups)], sem_l)

    def begin(k, _):
        acts_copy(k).start()
        probes_copy(k).start()
        return 0

    lax.fori_loop(0, steps, begin, 0)
    label_copy.start()

    def product(k):
        acts_copy(k).wait()
        probes_copy(k).wait()
        cols = pl.ds(pl.multiple_of(k * STEP, STEP), STEP)
        return jnp.dot(acts_v[:, cols], probes_v[cols], preferred_element_type=jnp.float32)

    acc[...] = product(0)

    def add(k, _):
        acc[...] += product(k)
        return 0

    lax.fori_loop(1, steps, add, 0)
    label_copy.wait()
    by_token = labels_v[...].T
    ids = lax.broadcasted_iota(jnp.int32, (LANES, classes), 1)
    loss = jnp.zeros((LANES, 1), jnp.float32)
    for g in range(groups):
        some = pl.ds(g * LANES, LANES)
        logits = acc[some]
        top = jnp.max(logits, axis=1, keepdims=True)
        expo = jnp.exp(logits - top)
        total = jnp.sum(expo, axis=1, keepdims=True)
        hit = ids == by_token[:, g : g + 1]
        probs = expo * (1.0 / total)
        resid_v[some] = jnp.where(hit, probs - 1.0, probs).astype(jnp.bfloat16)
        picked = jnp.sum(jnp.where(hit, logits, 0.0), axis=1, keepdims=True)
        loss += top + jnp.log(total) - picked
    loss_v[...] = jnp.full(loss_v.shape, jnp.sum(loss), jnp.float32)
    out_r = pltpu.make_async_copy(resid_v, resid_o, sem_o.at[0])
    out_r.start()
    out_l = pltpu.make_async_copy(loss_v, loss_o, sem_o.at[1])
    out_l.start()
    out_xl = pltpu.make_async_copy(loss_v, x0_o.at[pl.ds(half, SUB)], sem_o.at[2])
    out_xl.start()

    x, far, _, other, _ = place()
    mate = 1 - x
    base = rows // LANES * LANES
    span = prod.shape[1]
    outs = []
    for n, (chunk, dst) in enumerate(((far, x0_o.at[pl.ds(0, half)]), (other, e_o))):
        cols = pl.ds(pl.multiple_of(chunk * (2 * rows) + mate * base, LANES), span)
        prod[n] = lax.dot_general(acts_v[:, cols], resid_v[...], TN, preferred_element_type=jnp.float32) * factor
        shift = pl.multiple_of(mate * (rows - base), SUB)
        out = pltpu.make_async_copy(prod.at[n, pl.ds(shift, half)], dst, sem_o.at[3 + n])
        out.start()
        outs.append(out)
    for out in [out_r, out_l, out_xl, *outs]:
        out.wait()


def second_kernel(factor, acts, resid, loss, s3b, k3a, k3b, s2a, s2b, k2a, k2b, sob, koa, kob, sna, snb, kna, knb, acts_v, resid_v, prod, tail_v, sem_a, sem_r, sem_o):
    half, classes = s3b.shape
    rows = 2 * half
    wide = 2 * rows
    x, *chunks = place()
    ins = []
    for n, chunk in enumerate(chunks):
        cols = pl.ds(pl.multiple_of(chunk * wide, LANES), wide)
        ins.append(pltpu.make_async_copy(acts.at[:, cols], acts_v.at[n], sem_a.at[n]))
    in_r = pltpu.make_async_copy(resid, resid_v, sem_r.at[0])
    in_r.start()
    in_l = pltpu.make_async_copy(loss, tail_v.at[0], sem_r.at[1])
    in_l.start()
    for copy in ins:
        copy.start()
    tail_v[1] = jnp.zeros((SUB, classes), jnp.float32)
    in_l.wait()
    body, tail = pl.ds(0, half), pl.ds(half, SUB)
    tails = [
        pltpu.make_async_copy(tail_v.at[0], k3a.at[tail], sem_r.at[2]),
        pltpu.make_async_copy(tail_v.at[1], koa.at[tail], sem_r.at[3]),
    ]
    for copy in tails:
        copy.start()
    in_r.wait()
    places = ((None, s3b, k3a.at[body], k3b), (s2a, s2b, k2a, k2b), (None, sob, koa.at[body], kob), (sna, snb, kna, knb))
    outs = []
    block = 3 * LANES if wide % (3 * LANES) == 0 else LANES
    for n, dsts in enumerate(places):
        ins[n].wait()

        def piece(j, _, n=n):
            cols = pl.ds(pl.multiple_of(j * block, LANES), block)
            prod[n, cols] = lax.dot_general(acts_v[n, :, cols], resid_v[...], TN, preferred_element_type=jnp.float32) * factor
            return 0

        lax.fori_loop(0, wide // block, piece, 0)
        for q, dst in enumerate(dsts):
            if dst is None:
                continue
            col = 1 - x if q < 2 else x
            first = pl.multiple_of(col * rows + (q % 2) * half, SUB)
            out = pltpu.make_async_copy(prod.at[n, pl.ds(first, half)], dst, sem_o.at[n, q])
            out.start()
            outs.append(out)
    for out in [*tails, *outs]:
        out.wait()


def exchanged(acts, probes, labels):
    shards = lax.axis_size("dp")
    _, tok, wide = acts.shape
    classes = probes.shape[2]
    rows = wide // shards
    half = rows // 2
    count_all = tok * shards
    factor = 1.0 / count_all**0.5
    f32, bf16 = jnp.float32, jnp.bfloat16
    shape = jax.ShapeDtypeStruct
    dma = pltpu.SemaphoreType.DMA
    steps = wide // STEP
    span = -(-(rows % LANES + half) // LANES) * LANES
    long = half + SUB
    flops = 2 * tok * wide * classes

    resid, x0, e, loss = pl.pallas_call(
        functools.partial(first_kernel, factor),
        out_shape=(shape((tok, classes), bf16), shape((long, classes), f32), shape((half, classes), f32), shape((SUB, classes), f32)),
        in_specs=[ANY, ANY, ANY],
        out_specs=(ANY, ANY, ANY, ANY),
        scratch_shapes=[
            pltpu.VMEM((tok, wide), bf16),
            pltpu.VMEM((wide, classes), bf16),
            pltpu.VMEM((-(-tok // LANES // SUB) * SUB, LANES), jnp.int32),
            pltpu.VMEM((tok, classes), f32),
            pltpu.VMEM((tok, classes), bf16),
            pltpu.VMEM((2, span, classes), f32),
            pltpu.VMEM((SUB, classes), f32),
            dma((steps,)),
            dma((steps,)),
            dma,
            dma((5,)),
        ],
        cost_estimate=pl.CostEstimate(flops=flops, bytes_accessed=2 * wide * (tok + classes), transcendentals=tok * classes),
        name="logits",
    )(acts[0], probes[0], labels.reshape(tok // LANES, LANES))

    piece = shape((half, classes), f32)
    piece_long = shape((long, classes), f32)
    s3b, k3a, k3b, s2a, s2b, k2a, k2b, sob, koa, kob, sna, snb, kna, knb = pl.pallas_call(
        functools.partial(second_kernel, factor),
        out_shape=(piece, piece_long, piece, piece, piece, piece, piece, piece, piece_long, piece, piece, piece, piece, piece),
        in_specs=[ANY, ANY, ANY],
        out_specs=(ANY,) * 14,
        scratch_shapes=[
            pltpu.VMEM((LINE, tok, 2 * rows), bf16),
            pltpu.VMEM((tok, classes), bf16),
            pltpu.VMEM((LINE, 2 * rows, classes), f32),
            pltpu.VMEM((2, SUB, classes), f32),
            dma((LINE,)),
            dma((4,)),
            dma((LINE, 4)),
        ],
        cost_estimate=pl.CostEstimate(flops=flops, bytes_accessed=2 * wide * tok + 4 * wide * classes, transcendentals=0),
        name="terms",
    )(acts[0], resid, loss)

    across = [(i, i ^ 1) for i in range(shards)]
    pairs = [(2 * a + c, 2 * b + c) for a, b in ((0, 1), (1, 0), (2, 3), (3, 2)) for c in (0, 1)]
    inward = [(2 * a + c, 2 * b + c) for a, b in ((0, 1), (3, 2)) for c in (0, 1)]
    middle = [(2 * a + c, 2 * b + c) for a, b in ((1, 2), (2, 1)) for c in (0, 1)]

    def send(value, way):
        return lax.ppermute(value, "dp", way)

    x0r = send(x0, across)
    er = send(e, pairs)
    x1r = send(s3b, across)
    x2r = send(s2a, across)
    x3r = send(s2b, across)
    x4r = send(sob, across)
    x5r = send(snb, across)
    x6r = send(sna + er, across)
    y3a = k3a + x0r
    r1r = send(y3a, pairs)
    y3b = k3b + x1r
    r2r = send(y3b, inward)
    y2a = k2a + x2r
    r3r = send(y2a, inward)
    y2b = k2b + x3r
    r4r = send(y2b, inward)
    v3a = y3a + r1r
    m1r = send(v3a, middle)
    m2r = send(y3b + r2r, middle)
    m3r = send(y2a + r3r, middle)
    m4r = send(y2b + r4r, middle)
    r5r = send(kob + x4r + m2r, pairs)
    r6r = send(koa + m1r, pairs)
    low = kna + x6r + r6r[:half] + m3r
    high = knb + x5r + r5r + m4r
    total = v3a[half:, :1] + m1r[half:, :1] + r6r[half:, :1]
    losses = total[0] / jnp.float32(count_all)
    return (jnp.concatenate([low, high])[None], losses)


def per_device(acts, probes, labels):
    shards = lax.axis_size("dp")
    _, tok, wide = acts.shape
    rows = wide // shards
    fits = shards == 2 * LINE and tok % LANES == 0 and wide % STEP == 0 and 2 * rows % LANES == 0 and rows % (2 * SUB) == 0
    return (exchanged if fits else plain)(acts, probes, labels)


def solution(mesh):
    placed = (P("layer", "dp", None), P("layer", None, None), P("dp"))
    return jax.shard_map(
        per_device,
        mesh=mesh,
        in_specs=placed,
        out_specs=(P("layer", "dp", None), P("layer")),
        check_vma=False,
    )
```
